32 devices in a mesh: data: 2 (over x), seq: 4 (over z), dap: 4 (over y, core).
Axes of the slice: x: 2, y: 2, z: 4, core: 2. Of those that a mesh axis runs over, the one named last changes fastest.
Arguments:
- msa_act: bfloat16 [2048, 384, 256], P(('data', 'seq'), 'dap'), parts along dimension 0
- msa_mask: int32 [2048, 384], P('data'), parts along dimension 0
- pair_act: float32 [768, 384, 128], P(('data', 'dap')), parts along dimension 0
- ln_gamma: bfloat16 [256], replicated
- ln_beta: bfloat16 [256], replicated
- w_left: bfloat16 [256, 32], replicated
- b_left: bfloat16 [32], replicated
- w_right: bfloat16 [256, 32], replicated
- b_right: bfloat16 [32], replicated
- w_out: bfloat16 [1024, 128], replicated
- b_out: bfloat16 [128], replicated
Outputs:
- output 1: float32 [768, 384, 128], P(('data', 'dap')), parts along dimension 0
- output 2: bfloat16 [2048, 384, 256], P(('data', 'seq', 'dap')), parts along dimension 0
There are 2 independent parts. The reference program is written for one: setup_inputs(seed, part) draws one part's arguments, and reference() takes and returns one part's arrays. A program takes and returns all parts, laid end to end along the dimension named above; an argument that names none is the same for every part.
All inputs are finite; a program needn't handle non-finite values.
Results may differ from the reference program's by a relative error of at most 0.0107188.
Values are sent between devices in bfloat16 or wider.
A program may use at most 1 GiB of HBM per device.

```python
import math
import jax
import jax.numpy as jnp
from jax import lax

S = 1024
N = 384
CM = 256
CH = 32
CZ = 128
ROW_BLOCK = math.gcd(N, 16)


def setup_inputs(seed: int = 0, part: int = 0) -> dict:
    root_key = jax.random.key(seed)
    shared_root, part_root = jax.random.split(root_key)
    part_key = jax.random.fold_in(part_root, part)
    part_keys = jax.random.split(part_key, 5)
    weight_keys = jax.random.split(shared_root, 8)
    bias_scale = 0.5 * S ** -0.25
    msa_act = jax.random.normal(part_keys[0], (S, N, CM), jnp.float32).astype(jnp.bfloat16)
    col_level = jax.random.randint(part_keys[1], (N,), 8, 16)
    row_shift = jax.random.randint(part_keys[2], (S,), -2, 3)
    draw_mask = jax.random.randint(part_keys[3], (S, N), 0, 16)
    kept_mask = (draw_mask < col_level[None, :] + row_shift[:, None]).astype(jnp.int32)
    first_row = (jnp.arange(S) == 0).astype(jnp.int32)[:, None]
    msa_mask = jnp.maximum(kept_mask, first_row)
    pair_act = 0.5 * jax.random.normal(part_keys[4], (N, N, CZ), jnp.float32)
    ln_gamma = (1.0 + 0.3 * jax.random.normal(weight_keys[0], (CM,), jnp.float32)).astype(jnp.bfloat16)
    ln_beta = (bias_scale * jax.random.normal(weight_keys[1], (CM,), jnp.float32)).astype(jnp.bfloat16)
    w_left = (jax.random.normal(weight_keys[2], (CM, CH), jnp.float32) * CM ** -0.5).astype(jnp.bfloat16)
    b_left = (bias_scale * jax.random.normal(weight_keys[3], (CH,), jnp.float32)).astype(jnp.bfloat16)
    w_right = (jax.random.normal(weight_keys[4], (CM, CH), jnp.float32) * CM ** -0.5).astype(jnp.bfloat16)
    b_right = (bias_scale * jax.random.normal(weight_keys[5], (CH,), jnp.float32)).astype(jnp.bfloat16)
    w_out = (jax.random.normal(weight_keys[6], (CH * CH, CZ), jnp.float32) * (0.5 * math.sqrt(S) / CH)).astype(jnp.bfloat16)
    b_out = (0.25 * S * jax.random.normal(weight_keys[7], (CZ,), jnp.float32)).astype(jnp.bfloat16)
    return {'msa_act': msa_act, 'msa_mask': msa_mask, 'pair_act': pair_act, 'ln_gamma': ln_gamma, 'ln_beta': ln_beta, 'w_left': w_left, 'b_left': b_left, 'w_right': w_right, 'b_right': b_right, 'w_out': w_out, 'b_out': b_out}


def layer_norm(msa_act, ln_gamma, ln_beta):
    act_f32 = msa_act.astype(jnp.float32)
    mean_val = jnp.mean(act_f32, axis=-1, keepdims=True)
    centered = act_f32 - mean_val
    var_val = jnp.mean(centered * centered, axis=-1, keepdims=True)
    normed = centered * lax.rsqrt(var_val + 1e-5)
    return (normed * ln_gamma.astype(jnp.float32) + ln_beta.astype(jnp.float32)).astype(jnp.bfloat16)


def project(normed, weight, bias_vec, mask_f32):
    flat_act = normed.reshape(-1, normed.shape[-1])
    out_f32 = jnp.dot(flat_act, weight, preferred_element_type=jnp.float32) + bias_vec.astype(jnp.float32)
    return (out_f32.reshape(normed.shape[:-1] + (weight.shape[1],)) * mask_f32[:, :, None]).astype(jnp.bfloat16)


def reference(msa_act, msa_mask, pair_act, ln_gamma, ln_beta, w_left, b_left, w_right, b_right, w_out, b_out):
    normed = layer_norm(msa_act, ln_gamma, ln_beta)
    mask_f32 = msa_mask.astype(jnp.float32)
    left_proj = project(normed, w_left, b_left, mask_f32)
    right_proj = project(normed, w_right, b_right, mask_f32)
    right_f32 = right_proj.astype(jnp.float32)
    w_out3 = w_out.astype(jnp.float32).reshape(CH, CH, CZ)
    left_blocks = jnp.moveaxis(left_proj.astype(jnp.float32).reshape(S, N // ROW_BLOCK, ROW_BLOCK, CH), 1, 0)

    def row_block(left_blk):
        outer_blk = jnp.einsum('sic,sjd->icjd', left_blk, right_f32).astype(jnp.bfloat16)
        return jnp.einsum('icjd,cde->ije', outer_blk.astype(jnp.float32), w_out3)

    proj_sum = lax.map(row_block, left_blocks).reshape(N, N, CZ)
    pair_count = jnp.dot(mask_f32.T, mask_f32)
    pair_out = pair_act + (proj_sum + b_out.astype(jnp.float32)) / (1e-3 + pair_count)[:, :, None]
    return pair_out, msa_act
```

```python
import functools
import jax
import jax.numpy as jnp
from jax import lax
from jax.experimental import pallas as pl
from jax.experimental.pallas import tpu as pltpu
from jax.sharding import PartitionSpec as P

MESH = pl.DeviceIdType.MESH
BF16 = jnp.bfloat16
F32 = jnp.float32

NZ = 4
LOC_S = 256
LOC_R = 96
PAD_R = 128
N_RES = 384
C_M = 256
C_H = 32
C_Z = 128
RB = 8
N_RB = LOC_R // RB
N_Q = 4
N_TILES = N_RB * N_Q
LAG = 2
N_STEPS = N_TILES + 3 * LAG
P_SLOTS = 8
S_SLOTS = 4
D_CHUNK = 8
PRO_R = 16
PRO_S = 32


def project_kernel(m_ref, mask_ref, gamma_ref, beta_ref, w_ref, bias_ref, at_ref, bt_ref, xs_ref, bs_ref):
    gamma = gamma_ref[...].reshape(1, 1, C_M)
    beta = beta_ref[...].reshape(1, 1, C_M)

    def norm(step, carry):
        start = pl.multiple_of(step * PRO_S, PRO_S)
        x = m_ref[pl.ds(start, PRO_S)].astype(F32)
        mean = jnp.mean(x, axis=-1, keepdims=True)
        cent = x - mean
        var = jnp.mean(cent * cent, axis=-1, keepdims=True)
        y = cent * lax.rsqrt(var + 1e-5) * gamma + beta
        xs_ref[:, pl.ds(start, PRO_S), :] = jnp.swapaxes(y, 0, 1).astype(BF16)
        return carry

    lax.fori_loop(0, LOC_S // PRO_S, norm, 0)
    for r in range(PRO_R):
        t = lax.dot_general(w_ref[...], xs_ref[r], (((1,), (1,)), ((), ())), preferred_element_type=F32)
        t = (t + bias_ref[...]) * mask_ref[r:r + 1, :]
        at_ref[r * C_H:(r + 1) * C_H, :] = t[:C_H].astype(BF16)
        bs_ref[r] = t[C_H:]
    bt_ref[...] = jnp.swapaxes(bs_ref[...], 0, 1).astype(BF16)


def project(m, mask_t, gamma, beta, w_t, bias):
    return pl.pallas_call(
        project_kernel,
        grid=(LOC_R // PRO_R,),
        in_specs=[
            pl.BlockSpec((LOC_S, PRO_R, C_M), lambda i: (0, i, 0)),
            pl.BlockSpec((PRO_R, LOC_S), lambda i: (i, 0)),
            pl.BlockSpec((1, C_M), lambda i: (0, 0)),
            pl.BlockSpec((1, C_M), lambda i: (0, 0)),
            pl.BlockSpec((2 * C_H, C_M), lambda i: (0, 0)),
            pl.BlockSpec((2 * C_H, 1), lambda i: (0, 0)),
        ],
        out_specs=[
            pl.BlockSpec((PRO_R * C_H, LOC_S), lambda i: (i, 0)),
            pl.BlockSpec((C_H, PRO_R, LOC_S), lambda i: (0, i, 0)),
        ],
        out_shape=[
            jax.ShapeDtypeStruct((LOC_R * C_H, LOC_S), BF16),
            jax.ShapeDtypeStruct((C_H, LOC_R, LOC_S), BF16),
        ],
        scratch_shapes=[
            pltpu.VMEM((PRO_R, LOC_S, C_M), BF16),
            pltpu.VMEM((PRO_R, C_H, LOC_S), F32),
        ],
        compiler_params=pltpu.CompilerParams(vmem_limit_bytes=40 * 2**20),
        name="project",
    )(m, mask_t, gamma, beta, w_t, bias)


def main_kernel(m_hbm, at_ref, bt_hbm, wt_ref, inv_ref, bo_ref, z_hbm,
                zo_hbm, mo_hbm,
                b_all, o_buf, p_buf, from_left, from_right, to_right, to_left, z_in, z_out,
                b_send, b_recv, b_local, m_send, m_recv, m_local,
                r_send, r_recv, l_send, l_recv, zi_sem, zo_sem):
    data = lax.axis_index('data')
    z = lax.axis_index('seq')
    d = lax.axis_index('dap')
    core = lax.rem(d, 2)
    chip = lax.div(d, 2)
    sib = chip * 2 + (1 - core)
    far = (1 - chip) * 2 + core
    far_sib = (1 - chip) * 2 + (1 - core)

    def dev(seq, dap):
        return (data, seq, dap)

    barrier = pltpu.get_barrier_semaphore()
    for peer in (sib, far, far_sib):
        pl.semaphore_signal(barrier, inc=1, device_id=dev(z, peer), device_id_type=MESH)

    @pl.when(z > 0)
    def _():
        pl.semaphore_signal(barrier, inc=1, device_id=dev(z - 1, d), device_id_type=MESH)

    @pl.when(z < NZ - 1)
    def _():
        pl.semaphore_signal(barrier, inc=1, device_id=dev(z + 1, d), device_id_type=MESH)

    at_end = jnp.logical_or(z == 0, z == NZ - 1)
    pl.semaphore_wait(barrier, jnp.where(at_end, 4, 5))

    b_own = pltpu.make_async_copy(bt_hbm, b_all.at[0, :, pl.ds(0, LOC_R), :], b_local)
    b_own.start()

    def b_copy(src, q, peer):
        return pltpu.make_async_remote_copy(
            src_ref=src, dst_ref=b_all.at[q, :, pl.ds(0, LOC_R), :],
            send_sem=b_send.at[q], recv_sem=b_recv.at[q],
            device_id=dev(z, peer), device_id_type=MESH)

    b_sib = b_copy(bt_hbm, 1, sib)
    b_far = b_copy(bt_hbm, 2, far)
    b_relay = b_copy(b_all.at[2, :, pl.ds(0, LOC_R), :], 3, sib)
    b_far.start()
    b_sib.start()

    def m_copy(k, peer):
        rows = m_hbm.shape[0] // 4
        return pltpu.make_async_remote_copy(
            src_ref=m_hbm.at[pl.ds(peer * rows, rows)],
            dst_ref=mo_hbm.at[:, pl.ds(pl.multiple_of(d * LOC_R, LOC_R), LOC_R), :],
            send_sem=m_send.at[k], recv_sem=m_recv.at[k],
            device_id=dev(z, peer), device_id_type=MESH)

    rows = m_hbm.shape[0] // 4
    m_copies = [m_copy(0, sib), m_copy(1, far), m_copy(2, far_sib)]
    for cp in m_copies:
        cp.start()
    m_own = pltpu.make_async_copy(
        m_hbm.at[pl.ds(d * rows, rows)],
        mo_hbm.at[:, pl.ds(pl.multiple_of(d * LOC_R, LOC_R), LOC_R), :], m_local)
    m_own.start()

    b_all[:, :, LOC_R:, :] = jnp.zeros((N_Q, C_H, PAD_R - LOC_R, LOC_S), BF16)
    b_own.wait()

    def columns(q):
        c2 = lax.rem(core + lax.rem(q, 2), 2)
        y2 = lax.rem(chip + lax.div(q, 2), 2)
        return pl.multiple_of((2 * y2 + c2) * LOC_R, LOC_R)

    def tile_of(t):
        return lax.div(t, N_RB), lax.rem(t, N_RB)

    def compute(t):
        q, rb = tile_of(t)
        slot = lax.rem(t, P_SLOTS)
        a_blk = at_ref[pl.ds(pl.multiple_of(rb * RB * C_H, RB * C_H), RB * C_H), :]
        acc = [None] * (RB // 2)
        for ch in range(C_H // D_CHUNK):
            b_blk = b_all[q, ch * D_CHUNK:(ch + 1) * D_CHUNK].reshape(D_CHUNK * PAD_R, LOC_S)
            o = lax.dot_general(a_blk, b_blk, (((1,), (1,)), ((), ())), preferred_element_type=F32).astype(BF16)
            for i in range(RB):
                for dd in range(D_CHUNK):
                    o_buf[i // 2, dd * C_H:(dd + 1) * C_H, (i % 2) * PAD_R:(i % 2 + 1) * PAD_R] = (
                        o[i * C_H:(i + 1) * C_H, dd * PAD_R:(dd + 1) * PAD_R])
            w_blk = wt_ref[:, ch * D_CHUNK * C_H:(ch + 1) * D_CHUNK * C_H]
            for p in range(RB // 2):
                r = jnp.dot(w_blk, o_buf[p], preferred_element_type=F32)
                acc[p] = r if acc[p] is None else acc[p] + r
        for p in range(RB // 2):
            for i in range(2):
                p_buf[slot, 2 * p + i] = acc[p][:, i * PAD_R:(i + 1) * PAD_R].T[:LOC_R]

    def right_copy(t):
        slot = lax.rem(t, S_SLOTS)
        return pltpu.make_async_remote_copy(
            src_ref=to_right.at[slot], dst_ref=from_left.at[t],
            send_sem=r_send.at[slot], recv_sem=r_recv.at[t],
            device_id=dev(z + 1, d), device_id_type=MESH)

    def left_copy(t):
        slot = lax.rem(t, S_SLOTS)
        return pltpu.make_async_remote_copy(
            src_ref=to_left.at[slot], dst_ref=from_right.at[t],
            send_sem=l_send.at[slot], recv_sem=l_recv.at[t],
            device_id=dev(z - 1, d), device_id_type=MESH)

    def z_window(ref, t):
        q, rb = tile_of(t)
        return ref.at[pl.ds(pl.multiple_of(rb * RB, RB), RB), pl.ds(columns(q), LOC_R), :]

    def z_fetch(t):
        slot = lax.rem(t, 2)
        return pltpu.make_async_copy(z_window(z_hbm, t), z_in.at[slot], zi_sem.at[slot])

    def z_write(t):
        slot = lax.rem(t, 2)
        return pltpu.make_async_copy(z_out.at[slot], z_window(zo_hbm, t), zo_sem.at[slot])

    lag_right = z * LAG
    lag_left = (NZ - 1 - z) * LAG
    lag_end = jnp.maximum(lag_right, lag_left)

    def step(n, carry):
        @pl.when(n == N_RB)
        def _():
            b_sib.wait_recv()

        @pl.when(n == N_RB + 2)
        def _():
            b_far.wait_recv()
            b_relay.start()

        @pl.when(n == 3 * N_RB)
        def _():
            b_relay.wait_recv()

        @pl.when(n < N_TILES)
        def _():
            compute(n)

        tr = n - lag_right
        right_on = jnp.logical_and(tr >= 0, tr < N_TILES)
        tl = n - lag_left
        left_on = jnp.logical_and(tl >= 0, tl < N_TILES)
        send_right = jnp.logical_and(right_on, z < NZ - 1)
        send_left = jnp.logical_and(left_on, z > 0)

        @pl.when(jnp.logical_and(right_on, z > 0))
        def _():
            pltpu.make_async_remote_copy(
                src_ref=to_right.at[0], dst_ref=from_left.at[tr],
                send_sem=r_send.at[0], recv_sem=r_recv.at[tr],
                device_id=dev(z - 1, d), device_id_type=MESH).wait_recv()

        @pl.when(jnp.logical_and(left_on, z < NZ - 1))
        def _():
            pltpu.make_async_remote_copy(
                src_ref=to_left.at[0], dst_ref=from_right.at[tl],
                send_sem=l_send.at[0], recv_sem=l_recv.at[tl],
                device_id=dev(z + 1, d), device_id_type=MESH).wait_recv()

        @pl.when(jnp.logical_and(send_right, tr >= S_SLOTS))
        def _():
            right_copy(tr - S_SLOTS).wait_send()

        @pl.when(jnp.logical_and(send_left, tl >= S_SLOTS))
        def _():
            left_copy(tl - S_SLOTS).wait_send()

        @pl.when(jnp.logical_and(send_right, z == 0))
        def _():
            to_right[lax.rem(tr, S_SLOTS)] = p_buf[lax.rem(tr, P_SLOTS)].astype(BF16)

        @pl.when(jnp.logical_and(send_right, z > 0))
        def _():
            to_right[lax.rem(tr, S_SLOTS)] = (
                p_buf[lax.rem(tr, P_SLOTS)] + from_left[tr].astype(F32)).astype(BF16)

        @pl.when(jnp.logical_and(send_left, z == NZ - 1))
        def _():
            to_left[lax.rem(tl, S_SLOTS)] = p_buf[lax.rem(tl, P_SLOTS)].astype(BF16)

        @pl.when(jnp.logical_and(send_left, z < NZ - 1))
        def _():
            to_left[lax.rem(tl, S_SLOTS)] = (
                p_buf[lax.rem(tl, P_SLOTS)] + from_right[tl].astype(F32)).astype(BF16)

        @pl.when(send_right)
        def _():
            right_copy(tr).start()

        @pl.when(send_left)
        def _():
            left_copy(tl).start()

        te = n - lag_end

        @pl.when(jnp.logical_and(te >= -1, te < N_TILES - 1))
        def _():
            z_fetch(te + 1).start()

        @pl.when(jnp.logical_and(te >= 0, te < N_TILES))
        def _():
            q, rb = tile_of(te)
            slot = lax.rem(te, 2)
            z_fetch(te).wait()

            @pl.when(te >= 2)
            def _():
                z_write(te - 2).wait()

            def finish(i, total):
                inv = inv_ref[rb, pl.ds(columns(q), LOC_R), :]
                z_out[slot, i] = z_in[slot, i] + (total + bo_ref[...]) * inv[:, i:i + 1]

            p_slot = lax.rem(te, P_SLOTS)

            @pl.when(z == 0)
            def _():
                for i in range(RB):
                    finish(i, p_buf[p_slot, i] + from_right[te, i].astype(F32))

            @pl.when(z == NZ - 1)
            def _():
                for i in range(RB):
                    finish(i, p_buf[p_slot, i] + from_left[te, i].astype(F32))

            @pl.when(jnp.logical_and(z > 0, z < NZ - 1))
            def _():
                for i in range(RB):
                    finish(i, p_buf[p_slot, i] + from_left[te, i].astype(F32) + from_right[te, i].astype(F32))

            z_write(te).start()

        return carry

    lax.fori_loop(0, N_STEPS, step, 0)

    @pl.when(z < NZ - 1)
    def _():
        for k in range(S_SLOTS):
            right_copy(N_TILES - S_SLOTS + k).wait_send()

    @pl.when(z > 0)
    def _():
        for k in range(S_SLOTS):
            left_copy(N_TILES - S_SLOTS + k).wait_send()

    z_write(N_TILES - 2).wait()
    z_write(N_TILES - 1).wait()
    b_sib.wait_send()
    b_far.wait_send()
    b_relay.wait_send()
    m_own.wait()
    for cp in m_copies:
        cp.wait()


def combine(m, a_t, b_t, w_t, inv, b_out, pair):
    any_spec = pl.BlockSpec(memory_space=pl.ANY)
    vmem_spec = pl.BlockSpec(memory_space=pltpu.VMEM)
    dma = pltpu.SemaphoreType.DMA
    return pl.pallas_call(
        main_kernel,
        in_specs=[any_spec, vmem_spec, any_spec, vmem_spec, vmem_spec, vmem_spec, any_spec],
        out_specs=[any_spec, any_spec],
        out_shape=[
            jax.ShapeDtypeStruct((LOC_R, N_RES, C_Z), F32),
            jax.ShapeDtypeStruct((LOC_S // 4, N_RES, C_M), BF16),
        ],
        scratch_shapes=[
            pltpu.VMEM((N_Q, C_H, PAD_R, LOC_S), BF16),
            pltpu.VMEM((RB // 2, D_CHUNK * C_H, 2 * PAD_R), BF16),
            pltpu.VMEM((P_SLOTS, RB, LOC_R, C_Z), F32),
            pltpu.VMEM((N_TILES, RB, LOC_R, C_Z), BF16),
            pltpu.VMEM((N_TILES, RB, LOC_R, C_Z), BF16),
            pltpu.VMEM((S_SLOTS, RB, LOC_R, C_Z), BF16),
            pltpu.VMEM((S_SLOTS, RB, LOC_R, C_Z), BF16),
            pltpu.VMEM((2, RB, LOC_R, C_Z), F32),
            pltpu.VMEM((2, RB, LOC_R, C_Z), F32),
            dma((4,)), dma((4,)), dma, dma((3,)), dma((3,)), dma,
            dma((S_SLOTS,)), dma((N_TILES,)), dma((S_SLOTS,)), dma((N_TILES,)), dma((2,)), dma((2,)),
        ],
        compiler_params=pltpu.CompilerParams(
            collective_id=0, has_side_effects=True, vmem_limit_bytes=60 * 2**20),
        name="combine",
    )(m, a_t, b_t, w_t, inv, b_out, pair)


def solution(mesh):
    rep = P()
    in_specs = (P(('data', 'seq'), 'dap', None), P('data', None), P(('data', 'dap'), None, None)) + (rep,) * 8
    out_specs = (P(('data', 'dap'), None, None), P(('data', 'seq', 'dap'), None, None))

    def local_fn(m, mask, pair, ln_gamma, ln_beta, w_left, b_left, w_right, b_right, w_out, b_out):
        seq_idx = lax.axis_index('seq')
        dap_idx = lax.axis_index('dap')
        mask_cols = lax.dynamic_slice_in_dim(mask, dap_idx * LOC_R, LOC_R, axis=1)
        mask_t = lax.dynamic_slice_in_dim(mask_cols, seq_idx * LOC_S, LOC_S, axis=0).astype(F32).T
        w_t = jnp.concatenate([w_left, w_right], axis=1).T
        bias = jnp.concatenate([b_left, b_right]).astype(F32)[:, None]
        a_t, b_t = project(m, mask_t, ln_gamma.astype(F32)[None], ln_beta.astype(F32)[None], w_t, bias)
        count = jnp.einsum('si,sj->ij', mask_cols.astype(BF16), mask.astype(BF16), preferred_element_type=F32)
        inv = (1.0 / (1e-3 + count)).reshape(N_RB, RB, N_RES).transpose(0, 2, 1)
        wo_t = w_out.reshape(C_H, C_H, C_Z).transpose(2, 1, 0).reshape(C_Z, C_H * C_H)
        pair_out, msa_out = combine(m, a_t, b_t, wo_t, inv, b_out.astype(F32)[None], pair)
        return pair_out, msa_out

    return jax.shard_map(local_fn, mesh=mesh, in_specs=in_specs, out_specs=out_specs, check_vma=False)
```

```python
import jax
import jax.numpy as jnp
from jax import lax
from jax.experimental import pallas as pl
from jax.experimental.pallas import tpu as pltpu
from jax.sharding import PartitionSpec as P

MESH = pl.DeviceIdType.MESH
BF16 = jnp.bfloat16
F32 = jnp.float32

NZ = 4
N_SEQ = 1024
LOC_S = 256
LOC_R = 96
PAD_R = 128
N_RES = 384
C_M = 256
C_H = 32
C_Z = 128
RB = 8
N_RB = LOC_R // RB
N_Q = 4
N_BLOCKS = N_RB * N_Q
UR = 4
UPB = RB // UR
N_UNITS = N_BLOCKS * UPB
LAG = 3
N_STEPS = N_UNITS + 3 * LAG
P_SLOTS = 16
R_SLOTS = 16
S_SLOTS = 6
D_CHUNK = 8
PRO_R = 16
HALF_S = 128
PRO_S = 16
PITCH = 2 * LOC_S + 1


def main_kernel(m_hbm, mask_hbm, gamma_ref, beta_ref, bl_ref, br_ref, bo_ref, wl_ref, wr_ref, wo_ref, z_hbm,
                zo_ref, mo_ref,
                b_all, at_ref, o_buf, p_buf, inv_buf, from_left, from_right, to_right, to_left, z_in,
                mask_ref, mask_t, m_buf, xs_ref, bs_ref, wp_ref, wt_ref, bias_ref,
                b_send, b_recv, m_send, m_recv, m_local,
                r_send, r_recv, l_send, l_recv, zi_sem, mb_sem, mask_sem):
    data = lax.axis_index('data')
    z = lax.axis_index('seq')
    d = lax.axis_index('dap')
    core = lax.rem(d, 2)
    chip = lax.div(d, 2)
    sib = chip * 2 + (1 - core)
    far = (1 - chip) * 2 + core
    far_sib = (1 - chip) * 2 + (1 - core)

    def dev(seq, dap):
        return (data, seq, dap)

    barrier = pltpu.get_barrier_semaphore()
    for peer in (sib, far, far_sib):
        pl.semaphore_signal(barrier, inc=1, device_id=dev(z, peer), device_id_type=MESH)

    @pl.when(z > 0)
    def _():
        pl.semaphore_signal(barrier, inc=1, device_id=dev(z - 1, d), device_id_type=MESH)

    @pl.when(z < NZ - 1)
    def _():
        pl.semaphore_signal(barrier, inc=1, device_id=dev(z + 1, d), device_id_type=MESH)

    def m_fetch(k, half):
        return pltpu.make_async_copy(
            m_hbm.at[pl.ds(half * HALF_S, HALF_S), pl.ds(pl.multiple_of(k * PRO_R, PRO_R), PRO_R), :],
            m_buf.at[half], mb_sem.at[half])

    def mask_fetch(k):
        return pltpu.make_async_copy(
            mask_hbm.at[pl.ds(pl.multiple_of(k * 128, 128), 128)], mask_ref.at[lax.rem(k, 2)], mask_sem.at[lax.rem(k, 2)])

    mask_fetch(0).start()
    mask_fetch(1).start()
    m_fetch(0, 0).start()
    m_fetch(0, 1).start()

    def eye(n):
        return (lax.broadcasted_iota(jnp.int32, (n, n), 0) == lax.broadcasted_iota(jnp.int32, (n, n), 1))

    def column(ref):
        return jnp.sum(jnp.where(eye(C_H), ref[...].astype(F32).reshape(1, C_H), 0.0), axis=1, keepdims=True)

    wp_ref[:C_H] = wl_ref[...]
    wp_ref[C_H:] = wr_ref[...]
    bias_ref[:C_H] = column(bl_ref)
    bias_ref[C_H:] = column(br_ref)
    wo = jnp.swapaxes(wo_ref[...].astype(F32).reshape(C_H, C_H, C_Z), 0, 1).reshape(C_H * C_H, C_Z)
    wt_ref[...] = lax.dot_general(eye(C_Z).astype(F32).astype(BF16), wo.astype(BF16), (((1,), (1,)), ((), ())),
                                  preferred_element_type=F32).astype(BF16)
    gamma = gamma_ref[...].astype(F32).reshape(1, 1, C_M)
    beta = beta_ref[...].astype(F32).reshape(1, 1, C_M)
    bo = bo_ref[...].astype(F32).reshape(1, C_Z)

    b_all[:, :, LOC_R:, :] = jnp.zeros((N_Q, C_H, PAD_R - LOC_R, LOC_S), BF16)

    def flip(k, carry):
        mask_fetch(k).wait()
        mask_t[:, pl.ds(pl.multiple_of(k * 128, 128), 128)] = mask_ref[lax.rem(k, 2)].astype(F32).T

        @pl.when(k < N_SEQ // 128 - 2)
        def _():
            mask_fetch(k + 2).start()

        return carry

    lax.fori_loop(0, N_SEQ // 128, flip, 0)

    at_end = jnp.logical_or(z == 0, z == NZ - 1)
    pl.semaphore_wait(barrier, jnp.where(at_end, 4, 5))

    rows = m_hbm.shape[0] // 4
    m_place = mo_ref.at[:, pl.ds(pl.multiple_of(d * LOC_R, LOC_R), LOC_R), :]

    def m_copy(k, peer):
        return pltpu.make_async_remote_copy(
            src_ref=m_hbm.at[pl.ds(peer * rows, rows)], dst_ref=m_place,
            send_sem=m_send.at[k], recv_sem=m_recv.at[k],
            device_id=dev(z, peer), device_id_type=MESH)

    m_copies = [m_copy(0, sib), m_copy(1, far), m_copy(2, far_sib)]
    m_own = pltpu.make_async_copy(m_hbm.at[pl.ds(d * rows, rows)], m_place, m_local)

    def project(k, carry):
        for half in range(2):
            m_fetch(k, half).wait()

            def norm(step, c2):
                start = pl.multiple_of(step * PRO_S, PRO_S)
                x = m_buf[half, pl.ds(start, PRO_S)].astype(F32)
                mean = jnp.mean(x, axis=-1, keepdims=True)
                cent = x - mean
                var = jnp.mean(cent * cent, axis=-1, keepdims=True)
                y = cent * lax.rsqrt(var + 1e-5) * gamma + beta
                for s in range(PRO_S):
                    for lanes in range(2):
                        xs_ref[pl.ds(2 * (half * HALF_S + start + s) + lanes, PRO_R, stride=PITCH), :] = (
                            y[s, :, lanes * 128:(lanes + 1) * 128])
                return c2

            lax.fori_loop(0, HALF_S // PRO_S, norm, 0)

            @pl.when(k < LOC_R // PRO_R - 1)
            def _():
                m_fetch(k + 1, half).start()

        mask_rows = mask_t[pl.ds(pl.multiple_of(d * LOC_R + k * PRO_R, PRO_R), PRO_R),
                           pl.ds(pl.multiple_of(z * LOC_S, LOC_S), LOC_S)]
        for r in range(PRO_R):
            x = jnp.concatenate([xs_ref[pl.ds(r * PITCH + lanes, LOC_S, stride=2), :] for lanes in range(2)], axis=1)
            t = lax.dot_general(wp_ref[...], x.astype(BF16), (((1,), (1,)), ((), ())), preferred_element_type=F32)
            t = (t + bias_ref[...]) * mask_rows[r:r + 1]
            at_ref[pl.ds(pl.multiple_of((k * PRO_R + r) * C_H, C_H), C_H), :] = t[:C_H].astype(BF16)
            bs_ref[r] = t[C_H:]
        b_all[0, :, pl.ds(pl.multiple_of(k * PRO_R, PRO_R), PRO_R), :] = (
            jnp.swapaxes(bs_ref[...], 0, 1).astype(BF16))
        return carry

    lax.fori_loop(0, LOC_R // PRO_R, project, 0)

    def b_copy(src_q, q, peer):
        return pltpu.make_async_remote_copy(
            src_ref=b_all.at[src_q, :, pl.ds(0, LOC_R), :], dst_ref=b_all.at[q, :, pl.ds(0, LOC_R), :],
            send_sem=b_send.at[q], recv_sem=b_recv.at[q],
            device_id=dev(z, peer), device_id_type=MESH)

    b_sib = b_copy(0, 1, sib)
    b_far = b_copy(0, 2, far)
    b_relay = b_copy(2, 3, sib)

    def columns(q):
        c2 = lax.rem(core + lax.rem(q, 2), 2)
        y2 = lax.rem(chip + lax.div(q, 2), 2)
        return pl.multiple_of((2 * y2 + c2) * LOC_R, LOC_R)

    def block_of(b):
        return lax.div(b, N_RB), lax.rem(b, N_RB)

    def compute(b):
        q, rb = block_of(b)
        slot = lax.rem(b, P_SLOTS // UPB) * UPB
        a_blk = at_ref[pl.ds(pl.multiple_of(rb * RB * C_H, RB * C_H), RB * C_H), :]
        acc = [None] * (RB // 2)
        for ch in range(C_H // D_CHUNK):
            b_blk = b_all[q, ch * D_CHUNK:(ch + 1) * D_CHUNK].reshape(D_CHUNK * PAD_R, LOC_S)
            o = lax.dot_general(a_blk, b_blk, (((1,), (1,)), ((), ())), preferred_element_type=F32).astype(BF16)
            for i in range(RB):
                for dd in range(D_CHUNK):
                    o_buf[i // 2, dd * C_H:(dd + 1) * C_H, (i % 2) * PAD_R:(i % 2 + 1) * PAD_R] = (
                        o[i * C_H:(i + 1) * C_H, dd * PAD_R:(dd + 1) * PAD_R])
            w_blk = wt_ref[:, ch * D_CHUNK * C_H:(ch + 1) * D_CHUNK * C_H]
            for p in range(RB // 2):
                r = jnp.dot(w_blk, o_buf[p], preferred_element_type=F32)
                acc[p] = r if acc[p] is None else acc[p] + r
        for i in range(RB):
            p_buf[slot + i // UR, i % UR] = acc[i // 2][:, (i % 2) * PAD_R:(i % 2 + 1) * PAD_R].T[:LOC_R]
        row_mask = mask_t[pl.ds(pl.multiple_of(d * LOC_R + rb * RB, RB), RB), :].astype(BF16)
        col_mask = mask_t[pl.ds(columns(q), LOC_R), :].astype(BF16)
        count = lax.dot_general(col_mask, row_mask, (((1,), (1,)), ((), ())), preferred_element_type=F32)
        inv = 1.0 / (1e-3 + count)
        for u in range(UPB):
            inv_buf[slot + u] = inv[:, u * UR:(u + 1) * UR]

    def right_copy(t, peer):
        slot = lax.rem(t, S_SLOTS)
        return pltpu.make_async_remote_copy(
            src_ref=to_right.at[slot], dst_ref=from_left.at[lax.rem(t, R_SLOTS)],
            send_sem=r_send.at[slot], recv_sem=r_recv.at[lax.rem(t, R_SLOTS)],
            device_id=dev(peer, d), device_id_type=MESH)

    def left_copy(t, peer):
        slot = lax.rem(t, S_SLOTS)
        return pltpu.make_async_remote_copy(
            src_ref=to_left.at[slot], dst_ref=from_right.at[lax.rem(t, R_SLOTS)],
            send_sem=l_send.at[slot], recv_sem=l_recv.at[lax.rem(t, R_SLOTS)],
            device_id=dev(peer, d), device_id_type=MESH)

    def z_fetch(b):
        q, rb = block_of(b)
        slot = lax.rem(b, 2)
        return pltpu.make_async_copy(
            z_hbm.at[pl.ds(pl.multiple_of(rb * RB, RB), RB), pl.ds(columns(q), LOC_R), :],
            z_in.at[slot], zi_sem.at[slot])

    lag_right = z * LAG
    lag_left = (NZ - 1 - z) * LAG
    lag_end = jnp.maximum(lag_right, lag_left)

    z_fetch(0).start()
    compute(0)
    b_far.start()
    b_sib.start()
    for cp in m_copies:
        cp.start()
    m_own.start()

    def step(n, carry):
        tr = n - lag_right
        right_on = jnp.logical_and(tr >= 0, tr < N_UNITS)
        tl = n - lag_left
        left_on = jnp.logical_and(tl >= 0, tl < N_UNITS)
        send_right = jnp.logical_and(right_on, z < NZ - 1)
        send_left = jnp.logical_and(left_on, z > 0)

        @pl.when(jnp.logical_and(right_on, z > 0))
        def _():
            right_copy(tr, z - 1).wait_recv()

        @pl.when(jnp.logical_and(left_on, z < NZ - 1))
        def _():
            left_copy(tl, z + 1).wait_recv()

        @pl.when(jnp.logical_and(send_right, tr >= S_SLOTS))
        def _():
            right_copy(tr - S_SLOTS, z + 1).wait_send()

        @pl.when(jnp.logical_and(send_left, tl >= S_SLOTS))
        def _():
            left_copy(tl - S_SLOTS, z - 1).wait_send()

        @pl.when(jnp.logical_and(send_right, z == 0))
        def _():
            to_right[lax.rem(tr, S_SLOTS)] = p_buf[lax.rem(tr, P_SLOTS)].astype(BF16)

        @pl.when(jnp.logical_and(send_right, z > 0))
        def _():
            to_right[lax.rem(tr, S_SLOTS)] = (
                p_buf[lax.rem(tr, P_SLOTS)] + from_left[lax.rem(tr, R_SLOTS)].astype(F32)).astype(BF16)

        @pl.when(jnp.logical_and(send_left, z == NZ - 1))
        def _():
            to_left[lax.rem(tl, S_SLOTS)] = p_buf[lax.rem(tl, P_SLOTS)].astype(BF16)

        @pl.when(jnp.logical_and(send_left, z < NZ - 1))
        def _():
            to_left[lax.rem(tl, S_SLOTS)] = (
                p_buf[lax.rem(tl, P_SLOTS)] + from_right[lax.rem(tl, R_SLOTS)].astype(F32)).astype(BF16)

        @pl.when(send_right)
        def _():
            right_copy(tr, z + 1).start()

        @pl.when(send_left)
        def _():
            left_copy(tl, z - 1).start()

        te = n - lag_end

        @pl.when(jnp.logical_and(te >= 0, te < N_UNITS))
        def _():
            blk = lax.div(te, UPB)
            u = lax.rem(te, UPB)
            q, rb = block_of(blk)

            @pl.when(u == 0)
            def _():
                z_fetch(blk).wait()

                @pl.when(blk < N_BLOCKS - 1)
                def _():
                    z_fetch(blk + 1).start()

            p_slot = lax.rem(te, P_SLOTS)
            r_slot = lax.rem(te, R_SLOTS)
            row0 = rb * RB + u * UR

            def finish(i, total):
                inv = inv_buf[p_slot][:, i:i + 1]
                zo_ref[row0 + i, pl.ds(columns(q), LOC_R), :] = (
                    z_in[lax.rem(blk, 2), u * UR + i] + (total + bo) * inv)

            @pl.when(z == 0)
            def _():
                for i in range(UR):
                    finish(i, p_buf[p_slot, i] + from_right[r_slot, i].astype(F32))

            @pl.when(z == NZ - 1)
            def _():
                for i in range(UR):
                    finish(i, p_buf[p_slot, i] + from_left[r_slot, i].astype(F32))

            @pl.when(jnp.logical_and(z > 0, z < NZ - 1))
            def _():
                for i in range(UR):
                    finish(i, p_buf[p_slot, i] + from_left[r_slot, i].astype(F32) + from_right[r_slot, i].astype(F32))

        @pl.when(lax.rem(n, UPB) == 0)
        def _():
            nb = lax.div(n, UPB) + 1

            @pl.when(nb == N_RB)
            def _():
                b_sib.wait_recv()

            @pl.when(nb == N_RB + 2)
            def _():
                b_far.wait_recv()
                b_relay.start()

            @pl.when(nb == 3 * N_RB)
            def _():
                b_relay.wait_recv()

            @pl.when(nb < N_BLOCKS)
            def _():
                compute(nb)

        return carry

    lax.fori_loop(0, N_STEPS, step, 0)

    @pl.when(z < NZ - 1)
    def _():
        for k in range(S_SLOTS):
            right_copy(N_UNITS - S_SLOTS + k, z + 1).wait_send()

    @pl.when(z > 0)
    def _():
        for k in range(S_SLOTS):
            left_copy(N_UNITS - S_SLOTS + k, z - 1).wait_send()

    b_sib.wait_send()
    b_far.wait_send()
    b_relay.wait_send()
    m_own.wait()
    for cp in m_copies:
        cp.wait()


def combine(m, mask, gamma, beta, b_left, b_right, b_out, w_left, w_right, w_out, pair):
    any_spec = pl.BlockSpec(memory_space=pl.ANY)
    vmem_spec = pl.BlockSpec(memory_space=pltpu.VMEM)
    dma = pltpu.SemaphoreType.DMA
    return pl.pallas_call(
        main_kernel,
        in_specs=[any_spec, any_spec] + [vmem_spec] * 8 + [any_spec],
        out_specs=[vmem_spec, vmem_spec],
        out_shape=[
            pltpu.VMEM((LOC_R, N_RES, C_Z), F32),
            pltpu.VMEM((LOC_S // 4, N_RES, C_M), BF16),
        ],
        scratch_shapes=[
            pltpu.VMEM((N_Q, C_H, PAD_R, LOC_S), BF16),
            pltpu.VMEM((LOC_R * C_H, LOC_S), BF16),
            pltpu.VMEM((RB // 2, D_CHUNK * C_H, 2 * PAD_R), BF16),
            pltpu.VMEM((P_SLOTS, UR, LOC_R, C_Z), F32),
            pltpu.VMEM((P_SLOTS, LOC_R, UR), F32),
            pltpu.VMEM((R_SLOTS, UR, LOC_R, C_Z), BF16),
            pltpu.VMEM((R_SLOTS, UR, LOC_R, C_Z), BF16),
            pltpu.VMEM((S_SLOTS, UR, LOC_R, C_Z), BF16),
            pltpu.VMEM((S_SLOTS, UR, LOC_R, C_Z), BF16),
            pltpu.VMEM((2, RB, LOC_R, C_Z), F32),
            pltpu.VMEM((2, 128, N_RES), jnp.int32),
            pltpu.VMEM((N_RES, N_SEQ), F32),
            pltpu.VMEM((2, HALF_S, PRO_R, C_M), BF16),
            pltpu.VMEM((PRO_R * (PITCH + 1), 128), F32),
            pltpu.VMEM((PRO_R, C_H, LOC_S), F32),
            pltpu.VMEM((2 * C_H, C_M), BF16),
            pltpu.VMEM((C_Z, C_H * C_H), BF16),
            pltpu.VMEM((2 * C_H, 1), F32),
            dma((4,)), dma((4,)), dma((3,)), dma((3,)), dma,
            dma((S_SLOTS,)), dma((R_SLOTS,)), dma((S_SLOTS,)), dma((R_SLOTS,)), dma((2,)), dma((2,)), dma((2,)),
        ],
        compiler_params=pltpu.CompilerParams(
            collective_id=0, has_side_effects=True, vmem_limit_bytes=28 * 2**20),
        name="combine",
    )(m, mask, gamma, beta, b_left, b_right, b_out, w_left, w_right, w_out, pair)


def emit_kernel(z_ref, m_ref, zo_hbm, mo_hbm, sems):
    copies = []
    for k in range(8):
        zr = pl.ds(k * (LOC_R // 8), LOC_R // 8)
        mr = pl.ds(k * (LOC_S // 32), LOC_S // 32)
        copies.append(pltpu.make_async_copy(z_ref.at[zr], zo_hbm.at[zr], sems.at[k]))
        copies.append(pltpu.make_async_copy(m_ref.at[mr], mo_hbm.at[mr], sems.at[8 + k]))
    for cp in copies:
        cp.start()
    for cp in copies:
        cp.wait()


def emit(pair, msa):
    any_spec = pl.BlockSpec(memory_space=pl.ANY)
    vmem_spec = pl.BlockSpec(memory_space=pltpu.VMEM)
    pair = pltpu.with_memory_space_constraint(pair, pltpu.VMEM)
    msa = pltpu.with_memory_space_constraint(msa, pltpu.VMEM)
    return pl.pallas_call(
        emit_kernel,
        in_specs=[vmem_spec, vmem_spec],
        out_specs=[any_spec, any_spec],
        out_shape=[
            jax.ShapeDtypeStruct((LOC_R, N_RES, C_Z), F32),
            jax.ShapeDtypeStruct((LOC_S // 4, N_RES, C_M), BF16),
        ],
        scratch_shapes=[pltpu.SemaphoreType.DMA((16,))],
        compiler_params=pltpu.CompilerParams(vmem_limit_bytes=28 * 2**20),
        name="emit",
    )(pair, msa)


def solution(mesh):
    rep = P()
    in_specs = (P(('data', 'seq'), 'dap', None), P('data', None), P(('data', 'dap'), None, None)) + (rep,) * 8
    out_specs = (P(('data', 'dap'), None, None), P(('data', 'seq', 'dap'), None, None))

    def local_fn(m, mask, pair, ln_gamma, ln_beta, w_left, b_left, w_right, b_right, w_out, b_out):
        pair_out, msa_out = combine(m, mask, ln_gamma, ln_beta, b_left, b_right, b_out,
                                    w_left.T, w_right.T, w_out, pair)
        pair_out, msa_out = emit(pair_out, msa_out)
        return pair_out, msa_out

    return jax.shard_map(local_fn, mesh=mesh, in_specs=in_specs, out_specs=out_specs, check_vma=False)
```

```python
import jax
import jax.numpy as jnp
from jax import lax
from jax.experimental import pallas as pl
from jax.experimental.pallas import tpu as pltpu
from jax.sharding import PartitionSpec as P

MESH = pl.DeviceIdType.MESH
BF16 = jnp.bfloat16
F32 = jnp.float32

NZ = 4
N_SEQ = 1024
LOC_S = 256
LOC_R = 96
PAD_R = 128
N_RES = 384
C_M = 256
C_H = 32
C_Z = 128
RB = 8
N_RB = LOC_R // RB
N_Q = 4
N_BLOCKS = N_RB * N_Q
UR = 2
UPB = RB // UR
N_UNITS = N_BLOCKS * UPB
LAG = 5
N_STEPS = N_UNITS + 3 * LAG
P_SLOTS = 24
R_SLOTS = 16
S_SLOTS = 8
D_CHUNK = 8
PRO_R = 16
HALF_S = 128
M_SLOTS = 4
PRO_S = 64
PITCH = 2 * LOC_S + 1


def main_kernel(m_hbm, mask_hbm, gamma_ref, beta_ref, bl_ref, br_ref, bo_ref, wl_ref, wr_ref, wo_ref, z_hbm,
                zo_ref, mo_ref,
                b_all, at_ref, o_buf, p_buf, inv_buf, from_left, from_right, to_right, to_left, z_in,
                mask_ref, mask_t, m_buf, xs_ref, bs_ref, wp_ref, wt_ref, bias_ref,
                b_send, b_recv, m_send, m_recv, m_local,
                r_send, r_recv, l_send, l_recv, zi_sem, mb_sem, mask_sem):
    data = lax.axis_index('data')
    z = lax.axis_index('seq')
    d = lax.axis_index('dap')
    core = lax.rem(d, 2)
    chip = lax.div(d, 2)
    sib = chip * 2 + (1 - core)
    far = (1 - chip) * 2 + core
    far_sib = (1 - chip) * 2 + (1 - core)

    def dev(seq, dap):
        return (data, seq, dap)

    barrier = pltpu.get_barrier_semaphore()
    for peer in (sib, far, far_sib):
        pl.semaphore_signal(barrier, inc=1, device_id=dev(z, peer), device_id_type=MESH)

    @pl.when(z > 0)
    def _():
        pl.semaphore_signal(barrier, inc=1, device_id=dev(z - 1, d), device_id_type=MESH)

    @pl.when(z < NZ - 1)
    def _():
        pl.semaphore_signal(barrier, inc=1, device_id=dev(z + 1, d), device_id_type=MESH)

    def m_fetch(k, half):
        return pltpu.make_async_copy(
            m_hbm.at[pl.ds(half * HALF_S, HALF_S), pl.ds(pl.multiple_of(k * PRO_R, PRO_R), PRO_R), :],
            m_buf.at[lax.rem(2 * k + half, M_SLOTS)], mb_sem.at[lax.rem(2 * k + half, M_SLOTS)])

    def mask_rows_of(k):
        return pl.multiple_of(lax.rem(2 * z + k, N_SEQ // 128) * 128, 128)

    def mask_fetch(k):
        return pltpu.make_async_copy(
            mask_hbm.at[pl.ds(mask_rows_of(k), 128)], mask_ref.at[lax.rem(k, 2)], mask_sem.at[lax.rem(k, 2)])

    mask_fetch(0).start()
    mask_fetch(1).start()
    for k in range(M_SLOTS):
        m_fetch(k // 2, k % 2).start()

    def eye(n):
        return (lax.broadcasted_iota(jnp.int32, (n, n), 0) == lax.broadcasted_iota(jnp.int32, (n, n), 1))

    def column(ref):
        return jnp.sum(jnp.where(eye(C_H), ref[...].astype(F32).reshape(1, C_H), 0.0), axis=1, keepdims=True)

    wp_ref[:C_H] = wl_ref[...]
    wp_ref[C_H:] = wr_ref[...]
    bias_ref[:C_H] = column(bl_ref)
    bias_ref[C_H:] = column(br_ref)
    wo = jnp.swapaxes(wo_ref[...].astype(F32).reshape(C_H, C_H, C_Z), 0, 1).reshape(C_H * C_H, C_Z)
    wt_ref[...] = lax.dot_general(eye(C_Z).astype(F32).astype(BF16), wo.astype(BF16), (((1,), (1,)), ((), ())),
                                  preferred_element_type=F32).astype(BF16)
    gamma = gamma_ref[...].astype(F32).reshape(1, 1, C_M)
    beta = beta_ref[...].astype(F32).reshape(1, 1, C_M)
    bo = bo_ref[...].astype(F32).reshape(1, C_Z)

    b_all[:, :, LOC_R:, :] = jnp.zeros((N_Q, C_H, PAD_R - LOC_R, LOC_S), BF16)

    def flip(k):
        mask_fetch(k).wait()
        mask_t[:, pl.ds(mask_rows_of(k), 128)] = mask_ref[lax.rem(k, 2)].astype(F32).T

        @pl.when(k < N_SEQ // 128 - 2)
        def _():
            mask_fetch(k + 2).start()

    flip(jnp.int32(0))
    flip(jnp.int32(1))

    at_end = jnp.logical_or(z == 0, z == NZ - 1)
    pl.semaphore_wait(barrier, jnp.where(at_end, 4, 5))

    rows = m_hbm.shape[0] // 4
    m_place = mo_ref.at[:, pl.ds(pl.multiple_of(d * LOC_R, LOC_R), LOC_R), :]

    def m_copy(k, peer):
        return pltpu.make_async_remote_copy(
            src_ref=m_hbm.at[pl.ds(peer * rows, rows)], dst_ref=m_place,
            send_sem=m_send.at[k], recv_sem=m_recv.at[k],
            device_id=dev(z, peer), device_id_type=MESH)

    m_copies = [m_copy(0, sib), m_copy(1, far), m_copy(2, far_sib)]
    m_own = pltpu.make_async_copy(m_hbm.at[pl.ds(d * rows, rows)], m_place, m_local)

    def project(k, carry):
        for half in range(2):
            m_fetch(k, half).wait()

            def norm(step, c2):
                start = pl.multiple_of(step * PRO_S, PRO_S)
                x = m_buf[lax.rem(2 * k + half, M_SLOTS), pl.ds(start, PRO_S)].astype(F32)
                mean = jnp.mean(x, axis=-1, keepdims=True)
                cent = x - mean
                var = jnp.mean(cent * cent, axis=-1, keepdims=True)
                y = cent * lax.rsqrt(var + 1e-5) * gamma + beta
                for s in range(PRO_S):
                    for lanes in range(2):
                        xs_ref[pl.ds(2 * (half * HALF_S + start + s) + lanes, PRO_R, stride=PITCH), :] = (
                            y[s, :, lanes * 128:(lanes + 1) * 128])
                return c2

            lax.fori_loop(0, HALF_S // PRO_S, norm, 0)

            @pl.when(k < LOC_R // PRO_R - M_SLOTS // 2)
            def _():
                m_fetch(k + M_SLOTS // 2, half).start()

        mask_rows = mask_t[pl.ds(pl.multiple_of(d * LOC_R + k * PRO_R, PRO_R), PRO_R),
                           pl.ds(pl.multiple_of(z * LOC_S, LOC_S), LOC_S)]
        for r in range(PRO_R):
            x = jnp.concatenate([xs_ref[pl.ds(r * PITCH + lanes, LOC_S, stride=2), :] for lanes in range(2)], axis=1)
            t = lax.dot_general(wp_ref[...], x.astype(BF16), (((1,), (1,)), ((), ())), preferred_element_type=F32)
            t = (t + bias_ref[...]) * mask_rows[r:r + 1]
            at_ref[pl.ds(pl.multiple_of((k * PRO_R + r) * C_H, C_H), C_H), :] = t[:C_H].astype(BF16)
            bs_ref[r] = t[C_H:]
        b_all[0, :, pl.ds(pl.multiple_of(k * PRO_R, PRO_R), PRO_R), :] = (
            jnp.swapaxes(bs_ref[...], 0, 1).astype(BF16))
        flip(k + 2)
        return carry

    lax.fori_loop(0, LOC_R // PRO_R, project, 0)

    def b_copy(src_q, q, peer):
        return pltpu.make_async_remote_copy(
            src_ref=b_all.at[src_q, :, pl.ds(0, LOC_R), :], dst_ref=b_all.at[q, :, pl.ds(0, LOC_R), :],
            send_sem=b_send.at[q], recv_sem=b_recv.at[q],
            device_id=dev(z, peer), device_id_type=MESH)

    b_sib = b_copy(0, 1, sib)
    b_far = b_copy(0, 2, far)
    b_relay = b_copy(2, 3, sib)

    def columns(q):
        c2 = lax.rem(core + lax.rem(q, 2), 2)
        y2 = lax.rem(chip + lax.div(q, 2), 2)
        return pl.multiple_of((2 * y2 + c2) * LOC_R, LOC_R)

    def block_of(b):
        return lax.div(b, N_RB), lax.rem(b, N_RB)

    def compute(b):
        q, rb = block_of(b)
        slot = lax.rem(b, P_SLOTS // UPB) * UPB
        a_blk = at_ref[pl.ds(pl.multiple_of(rb * RB * C_H, RB * C_H), RB * C_H), :]
        acc = [None] * (RB // 2)
        for ch in range(C_H // D_CHUNK):
            b_blk = b_all[q, ch * D_CHUNK:(ch + 1) * D_CHUNK].reshape(D_CHUNK * PAD_R, LOC_S)
            o = lax.dot_general(a_blk, b_blk, (((1,), (1,)), ((), ())), preferred_element_type=F32).astype(BF16)
            for i in range(RB):
                for dd in range(D_CHUNK):
                    o_buf[i // 2, dd * C_H:(dd + 1) * C_H, (i % 2) * PAD_R:(i % 2 + 1) * PAD_R] = (
                        o[i * C_H:(i + 1) * C_H, dd * PAD_R:(dd + 1) * PAD_R])
            w_blk = wt_ref[:, ch * D_CHUNK * C_H:(ch + 1) * D_CHUNK * C_H]
            for p in range(RB // 2):
                r = jnp.dot(w_blk, o_buf[p], preferred_element_type=F32)
                acc[p] = r if acc[p] is None else acc[p] + r
        for i in range(RB):
            p_buf[slot + i // UR, i % UR] = acc[i // 2][:, (i % 2) * PAD_R:(i % 2 + 1) * PAD_R].T[:LOC_R]
        row_mask = mask_t[pl.ds(pl.multiple_of(d * LOC_R + rb * RB, RB), RB), :].astype(BF16)
        col_mask = mask_t[pl.ds(columns(q), LOC_R), :].astype(BF16)
        count = lax.dot_general(col_mask, row_mask, (((1,), (1,)), ((), ())), preferred_element_type=F32)
        inv = 1.0 / (1e-3 + count)
        for u in range(UPB):
            inv_buf[slot + u] = inv[:, u * UR:(u + 1) * UR]

    def right_copy(t, peer):
        slot = lax.rem(t, S_SLOTS)
        return pltpu.make_async_remote_copy(
            src_ref=to_right.at[slot], dst_ref=from_left.at[lax.rem(t, R_SLOTS)],
            send_sem=r_send.at[slot], recv_sem=r_recv.at[lax.rem(t, R_SLOTS)],
            device_id=dev(peer, d), device_id_type=MESH)

    def left_copy(t, peer):
        slot = lax.rem(t, S_SLOTS)
        return pltpu.make_async_remote_copy(
            src_ref=to_left.at[slot], dst_ref=from_right.at[lax.rem(t, R_SLOTS)],
            send_sem=l_send.at[slot], recv_sem=l_recv.at[lax.rem(t, R_SLOTS)],
            device_id=dev(peer, d), device_id_type=MESH)

    def z_fetch(b):
        q, rb = block_of(b)
        slot = lax.rem(b, 2)
        return pltpu.make_async_copy(
            z_hbm.at[pl.ds(pl.multiple_of(rb * RB, RB), RB), pl.ds(columns(q), LOC_R), :],
            z_in.at[slot], zi_sem.at[slot])

    lag_right = z * LAG
    lag_left = (NZ - 1 - z) * LAG
    lag_end = jnp.maximum(lag_right, lag_left)

    z_fetch(0).start()
    compute(0)
    b_far.start()
    b_sib.start()
    m_copies[0].start()
    m_own.start()

    def step(n, carry):
        tr = n - lag_right
        right_on = jnp.logical_and(tr >= 0, tr < N_UNITS)
        tl = n - lag_left
        left_on = jnp.logical_and(tl >= 0, tl < N_UNITS)
        send_right = jnp.logical_and(right_on, z < NZ - 1)
        send_left = jnp.logical_and(left_on, z > 0)

        @pl.when(jnp.logical_and(right_on, z > 0))
        def _():
            right_copy(tr, z - 1).wait_recv()

        @pl.when(jnp.logical_and(left_on, z < NZ - 1))
        def _():
            left_copy(tl, z + 1).wait_recv()

        @pl.when(jnp.logical_and(send_right, tr >= S_SLOTS))
        def _():
            right_copy(tr - S_SLOTS, z + 1).wait_send()

        @pl.when(jnp.logical_and(send_left, tl >= S_SLOTS))
        def _():
            left_copy(tl - S_SLOTS, z - 1).wait_send()

        @pl.when(jnp.logical_and(send_right, z == 0))
        def _():
            to_right[lax.rem(tr, S_SLOTS)] = p_buf[lax.rem(tr, P_SLOTS)].astype(BF16)

        @pl.when(jnp.logical_and(send_right, z > 0))
        def _():
            to_right[lax.rem(tr, S_SLOTS)] = (
                p_buf[lax.rem(tr, P_SLOTS)] + from_left[lax.rem(tr, R_SLOTS)].astype(F32)).astype(BF16)

        @pl.when(jnp.logical_and(send_left, z == NZ - 1))
        def _():
            to_left[lax.rem(tl, S_SLOTS)] = p_buf[lax.rem(tl, P_SLOTS)].astype(BF16)

        @pl.when(jnp.logical_and(send_left, z < NZ - 1))
        def _():
            to_left[lax.rem(tl, S_SLOTS)] = (
                p_buf[lax.rem(tl, P_SLOTS)] + from_right[lax.rem(tl, R_SLOTS)].astype(F32)).astype(BF16)

        @pl.when(send_right)
        def _():
            right_copy(tr, z + 1).start()

        @pl.when(send_left)
        def _():
            left_copy(tl, z - 1).start()

        te = n - lag_end

        @pl.when(jnp.logical_and(te >= 0, te < N_UNITS))
        def _():
            blk = lax.div(te, UPB)
            u = lax.rem(te, UPB)
            q, rb = block_of(blk)

            @pl.when(u == 0)
            def _():
                z_fetch(blk).wait()

                @pl.when(blk < N_BLOCKS - 1)
                def _():
                    z_fetch(blk + 1).start()

            p_slot = lax.rem(te, P_SLOTS)
            r_slot = lax.rem(te, R_SLOTS)
            row0 = rb * RB + u * UR

            def finish(i, total):
                inv = inv_buf[p_slot][:, i:i + 1]
                zo_ref[row0 + i, pl.ds(columns(q), LOC_R), :] = (
                    z_in[lax.rem(blk, 2), u * UR + i] + (total + bo) * inv)

            @pl.when(z == 0)
            def _():
                for i in range(UR):
                    finish(i, p_buf[p_slot, i] + from_right[r_slot, i].astype(F32))

            @pl.when(z == NZ - 1)
            def _():
                for i in range(UR):
                    finish(i, p_buf[p_slot, i] + from_left[r_slot, i].astype(F32))

            @pl.when(jnp.logical_and(z > 0, z < NZ - 1))
            def _():
                for i in range(UR):
                    finish(i, p_buf[p_slot, i] + from_left[r_slot, i].astype(F32) + from_right[r_slot, i].astype(F32))

        @pl.when(lax.rem(n, UPB) == 0)
        def _():
            nb = lax.div(n, UPB) + 1

            @pl.when(nb == N_RB)
            def _():
                b_sib.wait_recv()

            @pl.when(nb == N_RB - 2)
            def _():
                b_far.wait_recv()
                b_relay.start()
                m_copies[1].start()
                m_copies[2].start()

            @pl.when(nb == 3 * N_RB)
            def _():
                b_relay.wait_recv()

            @pl.when(nb < N_BLOCKS)
            def _():
                compute(nb)

        return carry

    lax.fori_loop(0, N_STEPS, step, 0)

    @pl.when(z < NZ - 1)
    def _():
        for k in range(S_SLOTS):
            right_copy(N_UNITS - S_SLOTS + k, z + 1).wait_send()

    @pl.when(z > 0)
    def _():
        for k in range(S_SLOTS):
            left_copy(N_UNITS - S_SLOTS + k, z - 1).wait_send()

    b_sib.wait_send()
    b_far.wait_send()
    b_relay.wait_send()
    m_own.wait()
    for cp in m_copies:
        cp.wait()


def combine(m, mask, gamma, beta, b_left, b_right, b_out, w_left, w_right, w_out, pair):
    any_spec = pl.BlockSpec(memory_space=pl.ANY)
    vmem_spec = pl.BlockSpec(memory_space=pltpu.VMEM)
    dma = pltpu.SemaphoreType.DMA
    return pl.pallas_call(
        main_kernel,
        in_specs=[any_spec, any_spec] + [vmem_spec] * 8 + [any_spec],
        out_specs=[vmem_spec, vmem_spec],
        out_shape=[
            pltpu.VMEM((LOC_R, N_RES, C_Z), F32),
            pltpu.VMEM((LOC_S // 4, N_RES, C_M), BF16),
        ],
        scratch_shapes=[
            pltpu.VMEM((N_Q, C_H, PAD_R, LOC_S), BF16),
            pltpu.VMEM((LOC_R * C_H, LOC_S), BF16),
            pltpu.VMEM((RB // 2, D_CHUNK * C_H, 2 * PAD_R), BF16),
            pltpu.VMEM((P_SLOTS, UR, LOC_R, C_Z), F32),
            pltpu.VMEM((P_SLOTS, LOC_R, UR), F32),
            pltpu.VMEM((R_SLOTS, UR, LOC_R, C_Z), BF16),
            pltpu.VMEM((R_SLOTS, UR, LOC_R, C_Z), BF16),
            pltpu.VMEM((S_SLOTS, UR, LOC_R, C_Z), BF16),
            pltpu.VMEM((S_SLOTS, UR, LOC_R, C_Z), BF16),
            pltpu.VMEM((2, RB, LOC_R, C_Z), F32),
            pltpu.VMEM((2, 128, N_RES), jnp.int32),
            pltpu.VMEM((N_RES, N_SEQ), F32),
            pltpu.VMEM((M_SLOTS, HALF_S, PRO_R, C_M), BF16),
            pltpu.VMEM((PRO_R * (PITCH + 1), 128), F32),
            pltpu.VMEM((PRO_R, C_H, LOC_S), F32),
            pltpu.VMEM((2 * C_H, C_M), BF16),
            pltpu.VMEM((C_Z, C_H * C_H), BF16),
            pltpu.VMEM((2 * C_H, 1), F32),
            dma((4,)), dma((4,)), dma((3,)), dma((3,)), dma,
            dma((S_SLOTS,)), dma((R_SLOTS,)), dma((S_SLOTS,)), dma((R_SLOTS,)), dma((2,)), dma((M_SLOTS,)), dma((2,)),
        ],
        compiler_params=pltpu.CompilerParams(
            collective_id=0, has_side_effects=True, vmem_limit_bytes=30 * 2**20),
        name="combine",
    )(m, mask, gamma, beta, b_left, b_right, b_out, w_left, w_right, w_out, pair)


def emit_kernel(z_ref, m_ref, zo_hbm, mo_hbm, sems):
    copies = []
    for k in range(8):
        zr = pl.ds(k * (LOC_R // 8), LOC_R // 8)
        mr = pl.ds(k * (LOC_S // 32), LOC_S // 32)
        copies.append(pltpu.make_async_copy(z_ref.at[zr], zo_hbm.at[zr], sems.at[k]))
        copies.append(pltpu.make_async_copy(m_ref.at[mr], mo_hbm.at[mr], sems.at[8 + k]))
    for cp in copies:
        cp.start()
    for cp in copies:
        cp.wait()


def emit(pair, msa):
    any_spec = pl.BlockSpec(memory_space=pl.ANY)
    vmem_spec = pl.BlockSpec(memory_space=pltpu.VMEM)
    pair = pltpu.with_memory_space_constraint(pair, pltpu.VMEM)
    msa = pltpu.with_memory_space_constraint(msa, pltpu.VMEM)
    return pl.pallas_call(
        emit_kernel,
        in_specs=[vmem_spec, vmem_spec],
        out_specs=[any_spec, any_spec],
        out_shape=[
            jax.ShapeDtypeStruct((LOC_R, N_RES, C_Z), F32),
            jax.ShapeDtypeStruct((LOC_S // 4, N_RES, C_M), BF16),
        ],
        scratch_shapes=[pltpu.SemaphoreType.DMA((16,))],
        compiler_params=pltpu.CompilerParams(vmem_limit_bytes=30 * 2**20),
        name="emit",
    )(pair, msa)


def solution(mesh):
    rep = P()
    in_specs = (P(('data', 'seq'), 'dap', None), P('data', None), P(('data', 'dap'), None, None)) + (rep,) * 8
    out_specs = (P(('data', 'dap'), None, None), P(('data', 'seq', 'dap'), None, None))

    def local_fn(m, mask, pair, ln_gamma, ln_beta, w_left, b_left, w_right, b_right, w_out, b_out):
        pair_out, msa_out = combine(m, mask, ln_gamma, ln_beta, b_left, b_right, b_out,
                                    w_left.T, w_right.T, w_out, pair)
        pair_out, msa_out = emit(pair_out, msa_out)
        return pair_out, msa_out

    return jax.shard_map(local_fn, mesh=mesh, in_specs=in_specs, out_specs=out_specs, check_vma=False)
```

```python
import jax
import jax.numpy as jnp
from jax import lax
from jax.experimental import pallas as pl
from jax.experimental.pallas import tpu as pltpu
from jax.sharding import PartitionSpec as P

MESH = pl.DeviceIdType.MESH
BF16 = jnp.bfloat16
F32 = jnp.float32

NZ = 4
N_SEQ = 1024
LOC_S = 256
LOC_R = 96
PAD_R = 128
N_RES = 384
C_M = 256
C_H = 32
C_Z = 128
RB = 8
N_RB = LOC_R // RB
N_Q = 4
N_BLOCKS = N_RB * N_Q
UR = 2
UPB = RB // UR
N_UNITS = N_BLOCKS * UPB
LAG = 4
N_STEPS = N_UNITS + 3 * LAG
P_SLOTS = 24
R_SLOTS = 16
S_SLOTS = 8
D_CHUNK = 8
PRO_R = 16
HALF_S = 128
M_SLOTS = 4
PRO_S = 64
PITCH = 2 * LOC_S + 1


def main_kernel(m_hbm, mask_hbm, gamma_ref, beta_ref, bl_ref, br_ref, bo_ref, wl_ref, wr_ref, wo_ref, z_hbm,
                zo_ref, mo_ref,
                b_all, at_ref, o_buf, r_acc, p_buf, inv_buf, from_left, from_right, to_right, to_left, z_in,
                mask_ref, mask_t, m_buf, xs_ref, bs_ref, wp_ref, wt_ref, bias_ref,
                b_send, b_recv, m_send, m_recv, m_local,
                r_send, r_recv, l_send, l_recv, zi_sem, mb_sem, mask_sem):
    data = lax.axis_index('data')
    z = lax.axis_index('seq')
    d = lax.axis_index('dap')
    core = lax.rem(d, 2)
    chip = lax.div(d, 2)
    sib = chip * 2 + (1 - core)
    far = (1 - chip) * 2 + core
    far_sib = (1 - chip) * 2 + (1 - core)

    def dev(seq, dap):
        return (data, seq, dap)

    barrier = pltpu.get_barrier_semaphore()
    for peer in (sib, far, far_sib):
        pl.semaphore_signal(barrier, inc=1, device_id=dev(z, peer), device_id_type=MESH)

    @pl.when(z > 0)
    def _():
        pl.semaphore_signal(barrier, inc=1, device_id=dev(z - 1, d), device_id_type=MESH)

    @pl.when(z < NZ - 1)
    def _():
        pl.semaphore_signal(barrier, inc=1, device_id=dev(z + 1, d), device_id_type=MESH)

    def m_fetch(k, half):
        return pltpu.make_async_copy(
            m_hbm.at[pl.ds(half * HALF_S, HALF_S), pl.ds(pl.multiple_of(k * PRO_R, PRO_R), PRO_R), :],
            m_buf.at[lax.rem(2 * k + half, M_SLOTS)], mb_sem.at[lax.rem(2 * k + half, M_SLOTS)])

    def mask_rows_of(k):
        return pl.multiple_of(lax.rem(2 * z + k, N_SEQ // 128) * 128, 128)

    def mask_fetch(k):
        return pltpu.make_async_copy(
            mask_hbm.at[pl.ds(mask_rows_of(k), 128)], mask_ref.at[lax.rem(k, 2)], mask_sem.at[lax.rem(k, 2)])

    mask_fetch(0).start()
    mask_fetch(1).start()
    for k in range(M_SLOTS):
        m_fetch(k // 2, k % 2).start()

    def eye(n):
        return (lax.broadcasted_iota(jnp.int32, (n, n), 0) == lax.broadcasted_iota(jnp.int32, (n, n), 1))

    def column(ref):
        return jnp.sum(jnp.where(eye(C_H), ref[...].astype(F32).reshape(1, C_H), 0.0), axis=1, keepdims=True)

    wp_ref[:C_H] = wl_ref[...]
    wp_ref[C_H:] = wr_ref[...]
    bias_ref[:C_H] = column(bl_ref)
    bias_ref[C_H:] = column(br_ref)
    wo = jnp.swapaxes(wo_ref[...].astype(F32).reshape(C_H, C_H, C_Z), 0, 1).reshape(C_H * C_H, C_Z)
    wt_ref[...] = lax.dot_general(eye(C_Z).astype(F32).astype(BF16), wo.astype(BF16), (((1,), (1,)), ((), ())),
                                  preferred_element_type=F32).astype(BF16)
    gamma = gamma_ref[...].astype(F32).reshape(1, 1, C_M)
    beta = beta_ref[...].astype(F32).reshape(1, 1, C_M)
    bo = bo_ref[...].astype(F32).reshape(1, C_Z)

    b_all[:, :, LOC_R:, :] = jnp.zeros((N_Q, C_H, PAD_R - LOC_R, LOC_S), BF16)

    def flip(k):
        mask_fetch(k).wait()
        mask_t[:, pl.ds(mask_rows_of(k), 128)] = mask_ref[lax.rem(k, 2)].astype(F32).T

        @pl.when(k < N_SEQ // 128 - 2)
        def _():
            mask_fetch(k + 2).start()

    flip(jnp.int32(0))
    flip(jnp.int32(1))

    at_end = jnp.logical_or(z == 0, z == NZ - 1)
    pl.semaphore_wait(barrier, jnp.where(at_end, 4, 5))

    rows = m_hbm.shape[0] // 4
    m_place = mo_ref.at[:, pl.ds(pl.multiple_of(d * LOC_R, LOC_R), LOC_R), :]

    def m_copy(k, peer):
        return pltpu.make_async_remote_copy(
            src_ref=m_hbm.at[pl.ds(peer * rows, rows)], dst_ref=m_place,
            send_sem=m_send.at[k], recv_sem=m_recv.at[k],
            device_id=dev(z, peer), device_id_type=MESH)

    m_copies = [m_copy(0, sib), m_copy(1, far), m_copy(2, far_sib)]
    m_own = pltpu.make_async_copy(m_hbm.at[pl.ds(d * rows, rows)], m_place, m_local)

    def project(k, carry):
        for half in range(2):
            m_fetch(k, half).wait()

            def norm(step, c2):
                start = pl.multiple_of(step * PRO_S, PRO_S)
                x = m_buf[lax.rem(2 * k + half, M_SLOTS), pl.ds(start, PRO_S)].astype(F32)
                mean = jnp.mean(x, axis=-1, keepdims=True)
                cent = x - mean
                var = jnp.mean(cent * cent, axis=-1, keepdims=True)
                y = cent * lax.rsqrt(var + 1e-5) * gamma + beta
                for s in range(PRO_S):
                    for lanes in range(2):
                        xs_ref[pl.ds(2 * (half * HALF_S + start + s) + lanes, PRO_R, stride=PITCH), :] = (
                            y[s, :, lanes * 128:(lanes + 1) * 128])
                return c2

            lax.fori_loop(0, HALF_S // PRO_S, norm, 0)

            @pl.when(k < LOC_R // PRO_R - M_SLOTS // 2)
            def _():
                m_fetch(k + M_SLOTS // 2, half).start()

        mask_rows = mask_t[pl.ds(pl.multiple_of(d * LOC_R + k * PRO_R, PRO_R), PRO_R),
                           pl.ds(pl.multiple_of(z * LOC_S, LOC_S), LOC_S)]
        for r in range(PRO_R):
            x = jnp.concatenate([xs_ref[pl.ds(r * PITCH + lanes, LOC_S, stride=2), :] for lanes in range(2)], axis=1)
            t = lax.dot_general(wp_ref[...], x.astype(BF16), (((1,), (1,)), ((), ())), preferred_element_type=F32)
            t = (t + bias_ref[...]) * mask_rows[r:r + 1]
            at_ref[pl.ds(pl.multiple_of((k * PRO_R + r) * C_H, C_H), C_H), :] = t[:C_H].astype(BF16)
            bs_ref[r] = t[C_H:]
        b_all[0, :, pl.ds(pl.multiple_of(k * PRO_R, PRO_R), PRO_R), :] = (
            jnp.swapaxes(bs_ref[...], 0, 1).astype(BF16))
        flip(k + 2)
        return carry

    lax.fori_loop(0, LOC_R // PRO_R, project, 0)

    def b_copy(src_q, q, peer):
        return pltpu.make_async_remote_copy(
            src_ref=b_all.at[src_q, :, pl.ds(0, LOC_R), :], dst_ref=b_all.at[q, :, pl.ds(0, LOC_R), :],
            send_sem=b_send.at[q], recv_sem=b_recv.at[q],
            device_id=dev(z, peer), device_id_type=MESH)

    b_sib = b_copy(0, 1, sib)
    b_far = b_copy(0, 2, far)
    b_relay = b_copy(2, 3, sib)

    def columns(q):
        c2 = lax.rem(core + lax.rem(q, 2), 2)
        y2 = lax.rem(chip + lax.div(q, 2), 2)
        return pl.multiple_of((2 * y2 + c2) * LOC_R, LOC_R)

    def block_of(b):
        return lax.div(b, N_RB), lax.rem(b, N_RB)

    def compute(b, ch):
        q, rb = block_of(b)
        a_blk = at_ref[pl.ds(pl.multiple_of(rb * RB * C_H, RB * C_H), RB * C_H), :]
        b_blk = b_all[q, pl.ds(ch * D_CHUNK, D_CHUNK)].reshape(D_CHUNK * PAD_R, LOC_S)
        o = lax.dot_general(a_blk, b_blk, (((1,), (1,)), ((), ())), preferred_element_type=F32).astype(BF16)
        for i in range(RB):
            for dd in range(D_CHUNK):
                o_buf[i // 2, dd * C_H:(dd + 1) * C_H, (i % 2) * PAD_R:(i % 2 + 1) * PAD_R] = (
                    o[i * C_H:(i + 1) * C_H, dd * PAD_R:(dd + 1) * PAD_R])
        w_blk = wt_ref[:, pl.ds(pl.multiple_of(ch * D_CHUNK * C_H, D_CHUNK * C_H), D_CHUNK * C_H)]
        for p in range(RB // 2):
            r_acc[p] = jnp.where(ch == 0, 0.0, r_acc[p]) + jnp.dot(w_blk, o_buf[p], preferred_element_type=F32)

        @pl.when(ch == C_H // D_CHUNK - 1)
        def _():
            slot = lax.rem(b, P_SLOTS // UPB) * UPB
            for i in range(RB):
                p_buf[slot + i // UR, i % UR] = r_acc[i // 2, :, (i % 2) * PAD_R:(i % 2 + 1) * PAD_R].T[:LOC_R]
            row_mask = mask_t[pl.ds(pl.multiple_of(d * LOC_R + rb * RB, RB), RB), :].astype(BF16)
            col_mask = mask_t[pl.ds(columns(q), LOC_R), :].astype(BF16)
            count = lax.dot_general(col_mask, row_mask, (((1,), (1,)), ((), ())), preferred_element_type=F32)
            inv = 1.0 / (1e-3 + count)
            for u in range(UPB):
                inv_buf[slot + u] = inv[:, u * UR:(u + 1) * UR]

    def right_copy(t, peer):
        slot = lax.rem(t, S_SLOTS)
        return pltpu.make_async_remote_copy(
            src_ref=to_right.at[slot], dst_ref=from_left.at[lax.rem(t, R_SLOTS)],
            send_sem=r_send.at[slot], recv_sem=r_recv.at[lax.rem(t, R_SLOTS)],
            device_id=dev(peer, d), device_id_type=MESH)

    def left_copy(t, peer):
        slot = lax.rem(t, S_SLOTS)
        return pltpu.make_async_remote_copy(
            src_ref=to_left.at[slot], dst_ref=from_right.at[lax.rem(t, R_SLOTS)],
            send_sem=l_send.at[slot], recv_sem=l_recv.at[lax.rem(t, R_SLOTS)],
            device_id=dev(peer, d), device_id_type=MESH)

    def z_fetch(b):
        q, rb = block_of(b)
        slot = lax.rem(b, 2)
        return pltpu.make_async_copy(
            z_hbm.at[pl.ds(pl.multiple_of(rb * RB, RB), RB), pl.ds(columns(q), LOC_R), :],
            z_in.at[slot], zi_sem.at[slot])

    lag_right = z * LAG
    lag_left = (NZ - 1 - z) * LAG
    lag_end = jnp.maximum(lag_right, lag_left)

    z_fetch(0).start()
    r_acc[...] = jnp.zeros(r_acc.shape, F32)

    def first_block(ch, carry):
        compute(jnp.int32(0), ch)
        return carry

    lax.fori_loop(0, UPB, first_block, 0)
    b_far.start()
    b_sib.start()
    m_copies[0].start()
    m_own.start()

    def step(n, carry):
        tr = n - lag_right
        right_on = jnp.logical_and(tr >= 0, tr < N_UNITS)
        tl = n - lag_left
        left_on = jnp.logical_and(tl >= 0, tl < N_UNITS)
        send_right = jnp.logical_and(right_on, z < NZ - 1)
        send_left = jnp.logical_and(left_on, z > 0)

        @pl.when(jnp.logical_and(right_on, z > 0))
        def _():
            right_copy(tr, z - 1).wait_recv()

        @pl.when(jnp.logical_and(left_on, z < NZ - 1))
        def _():
            left_copy(tl, z + 1).wait_recv()

        @pl.when(jnp.logical_and(send_right, tr >= S_SLOTS))
        def _():
            right_copy(tr - S_SLOTS, z + 1).wait_send()

        @pl.when(jnp.logical_and(send_left, tl >= S_SLOTS))
        def _():
            left_copy(tl - S_SLOTS, z - 1).wait_send()

        @pl.when(jnp.logical_and(send_right, z == 0))
        def _():
            to_right[lax.rem(tr, S_SLOTS)] = p_buf[lax.rem(tr, P_SLOTS)].astype(BF16)

        @pl.when(jnp.logical_and(send_right, z > 0))
        def _():
            to_right[lax.rem(tr, S_SLOTS)] = (
                p_buf[lax.rem(tr, P_SLOTS)] + from_left[lax.rem(tr, R_SLOTS)].astype(F32)).astype(BF16)

        @pl.when(jnp.logical_and(send_left, z == NZ - 1))
        def _():
            to_left[lax.rem(tl, S_SLOTS)] = p_buf[lax.rem(tl, P_SLOTS)].astype(BF16)

        @pl.when(jnp.logical_and(send_left, z < NZ - 1))
        def _():
            to_left[lax.rem(tl, S_SLOTS)] = (
                p_buf[lax.rem(tl, P_SLOTS)] + from_right[lax.rem(tl, R_SLOTS)].astype(F32)).astype(BF16)

        @pl.when(send_right)
        def _():
            right_copy(tr, z + 1).start()

        @pl.when(send_left)
        def _():
            left_copy(tl, z - 1).start()

        te = n - lag_end

        @pl.when(jnp.logical_and(te >= 0, te < N_UNITS))
        def _():
            blk = lax.div(te, UPB)
            u = lax.rem(te, UPB)
            q, rb = block_of(blk)

            @pl.when(u == 0)
            def _():
                z_fetch(blk).wait()

                @pl.when(blk < N_BLOCKS - 1)
                def _():
                    z_fetch(blk + 1).start()

            p_slot = lax.rem(te, P_SLOTS)
            r_slot = lax.rem(te, R_SLOTS)
            row0 = rb * RB + u * UR

            def finish(i, total):
                inv = inv_buf[p_slot][:, i:i + 1]
                zo_ref[row0 + i, pl.ds(columns(q), LOC_R), :] = (
                    z_in[lax.rem(blk, 2), u * UR + i] + (total + bo) * inv)

            @pl.when(z == 0)
            def _():
                for i in range(UR):
                    finish(i, p_buf[p_slot, i] + from_right[r_slot, i].astype(F32))

            @pl.when(z == NZ - 1)
            def _():
                for i in range(UR):
                    finish(i, p_buf[p_slot, i] + from_left[r_slot, i].astype(F32))

            @pl.when(jnp.logical_and(z > 0, z < NZ - 1))
            def _():
                for i in range(UR):
                    finish(i, p_buf[p_slot, i] + from_left[r_slot, i].astype(F32) + from_right[r_slot, i].astype(F32))

        nb = lax.div(n, UPB) + 1

        @pl.when(lax.rem(n, UPB) == 0)
        def _():

            @pl.when(nb == N_RB)
            def _():
                b_sib.wait_recv()

            @pl.when(nb == N_RB - 2)
            def _():
                b_far.wait_recv()
                b_relay.start()
                m_copies[1].start()
                m_copies[2].start()

            @pl.when(nb == 3 * N_RB)
            def _():
                b_relay.wait_recv()

        @pl.when(nb < N_BLOCKS)
        def _():
            compute(nb, lax.rem(n, UPB))

        return carry

    lax.fori_loop(0, N_STEPS, step, 0)

    @pl.when(z < NZ - 1)
    def _():
        for k in range(S_SLOTS):
            right_copy(N_UNITS - S_SLOTS + k, z + 1).wait_send()

    @pl.when(z > 0)
    def _():
        for k in range(S_SLOTS):
            left_copy(N_UNITS - S_SLOTS + k, z - 1).wait_send()

    b_sib.wait_send()
    b_far.wait_send()
    b_relay.wait_send()
    m_own.wait()
    for cp in m_copies:
        cp.wait()


def combine(m, mask, gamma, beta, b_left, b_right, b_out, w_left, w_right, w_out, pair):
    any_spec = pl.BlockSpec(memory_space=pl.ANY)
    vmem_spec = pl.BlockSpec(memory_space=pltpu.VMEM)
    dma = pltpu.SemaphoreType.DMA
    return pl.pallas_call(
        main_kernel,
        in_specs=[any_spec, any_spec] + [vmem_spec] * 8 + [any_spec],
        out_specs=[vmem_spec, vmem_spec],
        out_shape=[
            pltpu.VMEM((LOC_R, N_RES, C_Z), F32),
            pltpu.VMEM((LOC_S // 4, N_RES, C_M), BF16),
        ],
        scratch_shapes=[
            pltpu.VMEM((N_Q, C_H, PAD_R, LOC_S), BF16),
            pltpu.VMEM((LOC_R * C_H, LOC_S), BF16),
            pltpu.VMEM((RB // 2, D_CHUNK * C_H, 2 * PAD_R), BF16),
            pltpu.VMEM((RB // 2, C_Z, 2 * PAD_R), F32),
            pltpu.VMEM((P_SLOTS, UR, LOC_R, C_Z), F32),
            pltpu.VMEM((P_SLOTS, LOC_R, UR), F32),
            pltpu.VMEM((R_SLOTS, UR, LOC_R, C_Z), BF16),
            pltpu.VMEM((R_SLOTS, UR, LOC_R, C_Z), BF16),
            pltpu.VMEM((S_SLOTS, UR, LOC_R, C_Z), BF16),
            pltpu.VMEM((S_SLOTS, UR, LOC_R, C_Z), BF16),
            pltpu.VMEM((2, RB, LOC_R, C_Z), F32),
            pltpu.VMEM((2, 128, N_RES), jnp.int32),
            pltpu.VMEM((N_RES, N_SEQ), F32),
            pltpu.VMEM((M_SLOTS, HALF_S, PRO_R, C_M), BF16),
            pltpu.VMEM((PRO_R * (PITCH + 1), 128), F32),
            pltpu.VMEM((PRO_R, C_H, LOC_S), F32),
            pltpu.VMEM((2 * C_H, C_M), BF16),
            pltpu.VMEM((C_Z, C_H * C_H), BF16),
            pltpu.VMEM((2 * C_H, 1), F32),
            dma((4,)), dma((4,)), dma((3,)), dma((3,)), dma,
            dma((S_SLOTS,)), dma((R_SLOTS,)), dma((S_SLOTS,)), dma((R_SLOTS,)), dma((2,)), dma((M_SLOTS,)), dma((2,)),
        ],
        compiler_params=pltpu.CompilerParams(
            collective_id=0, has_side_effects=True, vmem_limit_bytes=30 * 2**20),
        name="combine",
    )(m, mask, gamma, beta, b_left, b_right, b_out, w_left, w_right, w_out, pair)


def emit_kernel(z_ref, m_ref, zo_hbm, mo_hbm, sems):
    copies = []
    for k in range(8):
        zr = pl.ds(k * (LOC_R // 8), LOC_R // 8)
        mr = pl.ds(k * (LOC_S // 32), LOC_S // 32)
        copies.append(pltpu.make_async_copy(z_ref.at[zr], zo_hbm.at[zr], sems.at[k]))
        copies.append(pltpu.make_async_copy(m_ref.at[mr], mo_hbm.at[mr], sems.at[8 + k]))
    for cp in copies:
        cp.start()
    for cp in copies:
        cp.wait()


def emit(pair, msa):
    any_spec = pl.BlockSpec(memory_space=pl.ANY)
    vmem_spec = pl.BlockSpec(memory_space=pltpu.VMEM)
    pair = pltpu.with_memory_space_constraint(pair, pltpu.VMEM)
    msa = pltpu.with_memory_space_constraint(msa, pltpu.VMEM)
    return pl.pallas_call(
        emit_kernel,
        in_specs=[vmem_spec, vmem_spec],
        out_specs=[any_spec, any_spec],
        out_shape=[
            jax.ShapeDtypeStruct((LOC_R, N_RES, C_Z), F32),
            jax.ShapeDtypeStruct((LOC_S // 4, N_RES, C_M), BF16),
        ],
        scratch_shapes=[pltpu.SemaphoreType.DMA((16,))],
        compiler_params=pltpu.CompilerParams(vmem_limit_bytes=30 * 2**20),
        name="emit",
    )(pair, msa)


def solution(mesh):
    rep = P()
    in_specs = (P(('data', 'seq'), 'dap', None), P('data', None), P(('data', 'dap'), None, None)) + (rep,) * 8
    out_specs = (P(('data', 'dap'), None, None), P(('data', 'seq', 'dap'), None, None))

    def local_fn(m, mask, pair, ln_gamma, ln_beta, w_left, b_left, w_right, b_right, w_out, b_out):
        pair_out, msa_out = combine(m, mask, ln_gamma, ln_beta, b_left, b_right, b_out,
                                    w_left.T, w_right.T, w_out, pair)
        pair_out, msa_out = emit(pair_out, msa_out)
        return pair_out, msa_out

    return jax.shard_map(local_fn, mesh=mesh, in_specs=in_specs, out_specs=out_specs, check_vma=False)
```
